32 devices in a mesh: pool: 4 (over z), fft: 8 (over y, x, core).
Axes of the slice: x: 2, y: 2, z: 4, core: 2. Of those that a mesh axis runs over, the one named last changes fastest.
Arguments:
- orbitals: bfloat16 [4, 2, 1, 160, 25600], P('pool', None, None, 'fft'), may hold values from -6 to 6
- stick_map: int32 [16000], replicated, may hold values from -1 to 25599, as said below
- kpoint_grid: int32 [4, 3], replicated, may hold values from 0 to 3, as said below
Outputs:
- exchange_action: bfloat16 [4, 2, 1, 160, 25600], P('pool', None, None, 'fft')
The draws below stay inside these ranges and needn't reach their ends.
Inputs may be any that keep to these rules, and one draw needn't show every extreme that they name: `stick_map`: entries other than -1 are distinct columns. Slots come in blocks of 2000 per index of fft; in each block at least half of the slots are live, and in every draw some block has all 2000 live. `kpoint_grid`: rows are distinct.
All inputs are finite; a program needn't handle non-finite values.
Results may differ from the reference program's by a relative error of at most 0.011.
Values may be sent and summed in bfloat16 or wider, within the bound.
A program may use at most 64 MiB of HBM per device.

```python
import math
import jax
import jax.numpy as jnp
from jax import lax

NG = 160
BANDS = 1
KMESH = 4
KPOINTS = 4
STICKS_DEV = 2000
STICKS_ALL = 16000


def draw_stick_map(key, part):
    devices = STICKS_ALL // STICKS_DEV
    key_counts = jax.random.fold_in(key, 11)
    key_full = jax.random.fold_in(key, 12)
    key_order = jax.random.fold_in(key, 13)
    counts = jax.random.randint(key_counts, (devices,), STICKS_DEV // 2, STICKS_DEV + 1)
    full_device = jax.random.randint(key_full, (), 0, devices)
    device_ids = jnp.arange(devices, dtype=jnp.int32)
    counts = jnp.where(device_ids == full_device, STICKS_DEV, counts).astype(jnp.int32)
    offsets = jnp.cumsum(counts) - counts
    shuffled = jax.random.permutation(key_order, NG * NG).astype(jnp.int32)
    column_x = shuffled % NG
    column_y = shuffled // NG
    signed_x = jnp.where(column_x >= NG // 2, column_x - NG, column_x)
    signed_y = jnp.where(column_y >= NG // 2, column_y - NG, column_y)
    outside = (signed_x * signed_x + signed_y * signed_y > NG // 2 * (NG // 2)).astype(jnp.int32)
    ordering = jnp.argsort(outside, stable=True)
    columns = shuffled[ordering]
    slot_ids = jnp.arange(STICKS_DEV, dtype=jnp.int32)
    positions = offsets[:, None] + slot_ids[None, :]
    positions = jnp.minimum(positions, NG * NG - 1)
    chosen = columns[positions]
    filled = jnp.where(slot_ids[None, :] < counts[:, None], chosen, -1)
    return filled.reshape(STICKS_ALL).astype(jnp.int32)


def draw_kpoint_grid(key, part):
    picked = jax.random.permutation(jax.random.fold_in(key, 21), KMESH * KMESH * KMESH)[:KPOINTS].astype(jnp.int32)
    first = picked // (KMESH * KMESH)
    second = picked // KMESH % KMESH
    third = picked % KMESH
    return jnp.stack([first, second, third], axis=1).astype(jnp.int32)


def steps_of(key, extent, split, low, largest):
    def one(position, shards_of):
        heights = jax.random.uniform(jax.random.fold_in(jax.random.fold_in(key, 6), position), (shards_of,), jnp.float32, low / len(split), largest / len(split))
        return jnp.repeat(jnp.exp(heights), extent[position] // shards_of).reshape((-1,) + (1,) * (len(extent) - position - 1))

    level = one(*split[0])
    for cut in split[1:]:
        level = level * one(*cut)
    return level


def noise(stream_key, shape, spread, bound, cuts=(), kind=jnp.bfloat16):
    values = jax.random.normal(stream_key, shape, jnp.float32) * spread
    if len(cuts) > 0:
        values = steps_of(stream_key, shape, cuts, -0.22, 0.18) * values
    return jnp.clip(values, min=-bound, max=bound).astype(kind)


def setup_inputs(seed: int = 0) -> dict:
    seeds = jax.random.split(jax.random.key(seed), 4)
    return {
        "orbitals": noise(seeds[0], (KPOINTS, 2, BANDS, NG, NG * NG), 1.0, 6.0, ((0, 4), (3, 8))),
        "stick_map": draw_stick_map(jax.random.fold_in(seeds[3], 71), 0),
        "kpoint_grid": draw_kpoint_grid(jax.random.fold_in(seeds[3], 71), 0),
    }


SPACING_BOHR = 0.1875
SCREENING = 0.106


def dft_table(grid_size, orientation):
    positions = jnp.arange(grid_size, dtype=jnp.int32)
    product = (positions[:, None] * positions[None, :]) % grid_size
    angle = product.astype(jnp.float32) * (2.0 * math.pi / grid_size)
    cosine = jnp.cos(angle)
    sine = orientation * jnp.sin(angle)
    upper = jnp.stack([cosine, sine], axis=1)
    lower = jnp.stack([-sine, cosine], axis=1)
    return jnp.stack([upper, lower], axis=0).astype(jnp.bfloat16)


def signed(frequency, grid_size):
    return jnp.where(frequency >= grid_size // 2, frequency - grid_size, frequency)


def kernel_table(columns, shift_q, grid_size):
    live_slot = columns >= 0
    column_ids = jnp.where(live_slot, columns, 0)
    freq_x = signed(column_ids % grid_size, grid_size)
    freq_y = signed(column_ids // grid_size, grid_size)
    freq_z = signed(jnp.arange(grid_size, dtype=jnp.int32), grid_size)
    radius = grid_size // 2
    inside = (freq_x * freq_x + freq_y * freq_y)[None, :] + (freq_z * freq_z)[:, None] <= radius * radius
    inside = jnp.logical_and(inside, live_slot[None, :])
    wave_x = freq_x.astype(jnp.float32) + shift_q[0]
    wave_y = freq_y.astype(jnp.float32) + shift_q[1]
    wave_z = freq_z.astype(jnp.float32) + shift_q[2]
    square = (wave_z * wave_z)[:, None] + (wave_x * wave_x + wave_y * wave_y)[None, :]
    cell = SPACING_BOHR * grid_size
    exponent = (math.pi * math.pi) * square / (cell * cell * SCREENING * SCREENING)
    weights = (cell * cell / math.pi) * (-jnp.expm1(-exponent)) / square / (float(grid_size) ** 3)
    return jnp.where(inside, weights, 0.0).astype(jnp.float32)


def momentum(kpoint_grid, pool_rank, pool_count):
    pool_rows = jnp.arange(pool_count, dtype=jnp.int32)
    earlier = (pool_rank + pool_count - 1) % pool_count
    current = jnp.sum(jnp.where((pool_rows == pool_rank)[:, None], kpoint_grid, 0), axis=0)
    previous = jnp.sum(jnp.where((pool_rows == earlier)[:, None], kpoint_grid, 0), axis=0)
    return (current - previous).astype(jnp.float32) / KMESH


def pair_density(own_bands, received):
    band_count = own_bands.shape[1]
    real_own = own_bands[0].astype(jnp.float32)[:, None]
    imag_own = own_bands[1].astype(jnp.float32)[:, None]
    real_recv = received[0].astype(jnp.float32)[None]
    imag_recv = received[1].astype(jnp.float32)[None]
    real_part = real_recv * real_own + imag_recv * imag_own
    imag_part = real_recv * imag_own - imag_recv * real_own
    stacked = jnp.stack([real_part, imag_part], axis=2)
    return stacked.reshape((band_count * band_count, 2) + own_bands.shape[2:]).astype(jnp.bfloat16)


def action_of(received, field):
    band_count = received.shape[1]
    field = field.reshape((band_count, band_count) + field.shape[1:])
    real_recv = received[0].astype(jnp.float32)[None]
    imag_recv = received[1].astype(jnp.float32)[None]
    real_field = field[:, :, 0]
    imag_field = field[:, :, 1]
    real_part = -jnp.sum(real_recv * real_field - imag_recv * imag_field, axis=1)
    imag_part = -jnp.sum(real_recv * imag_field + imag_recv * real_field, axis=1)
    return jnp.stack([real_part, imag_part], axis=0).astype(jnp.bfloat16)


def apply_table(data, table, form):
    return jnp.einsum(form, data.astype(jnp.float32), table.astype(jnp.float32), precision=lax.Precision.HIGHEST)


def column_pass(picked, weights, forward, backward):
    spectrum = apply_table(picked, forward, "pczs,czdk->pdks")
    scaled = (spectrum * weights).astype(jnp.bfloat16)
    return apply_table(scaled, backward, "pczs,czdk->pdks").astype(jnp.bfloat16)


def reference(orbitals, stick_map, kpoint_grid):
    pool_count = orbitals.shape[0]
    grid_size = orbitals.shape[3]
    orbitals = orbitals.reshape(orbitals.shape[:4] + (grid_size, grid_size))
    forward = dft_table(grid_size, -1.0)
    backward = dft_table(grid_size, 1.0)
    live_slot = stick_map >= 0
    column_ids = jnp.where(live_slot, stick_map, 0).astype(jnp.int32)

    def one_pool(pool_rank):
        own_bands = lax.dynamic_index_in_dim(orbitals, pool_rank, 0, keepdims=False)
        earlier = ((pool_rank + pool_count - 1) % pool_count).astype(jnp.int32)
        received = lax.dynamic_index_in_dim(orbitals, earlier, 0, keepdims=False)
        density = pair_density(own_bands, received)
        along_x = apply_table(density, forward, "pczyx,cxek->pezyk").astype(jnp.bfloat16)
        along_y = apply_table(along_x, forward, "pczyx,cyek->pezkx").astype(jnp.bfloat16)
        flattened = along_y.reshape(along_y.shape[:3] + (grid_size * grid_size,))
        picked = jnp.where(live_slot, jnp.take(flattened, column_ids, axis=3), 0).astype(jnp.bfloat16)
        weights = kernel_table(stick_map, momentum(kpoint_grid, pool_rank, pool_count), grid_size)
        returned = column_pass(picked, weights, forward, backward)
        merged = jnp.zeros_like(flattened).at[:, :, :, column_ids].add(jnp.where(live_slot, returned, 0).astype(jnp.bfloat16))
        back_y = apply_table(merged.reshape(along_y.shape), backward, "pczkx,ckey->pezyx").astype(jnp.bfloat16)
        field = apply_table(back_y, backward, "pczyk,ckex->pezyx")
        result = action_of(received, field)
        return result.reshape(result.shape[:3] + (grid_size * grid_size,))

    return lax.map(one_pool, jnp.arange(pool_count, dtype=jnp.int32))
```

```python
import functools
import math

import jax
import jax.numpy as jnp
import numpy as np
from jax import lax
from jax.experimental import pallas as pl
from jax.experimental.pallas import tpu as pltpu
from jax.sharding import PartitionSpec as P

KMESH = 4
SPACING_BOHR = 0.1875
SCREENING = 0.106
LANES = 128
BF = jnp.bfloat16
F32 = jnp.float32


def up(value, unit):
    return -(-value // unit) * unit


def lane_order(grid):
    half = LANES // 2
    low = np.concatenate([np.arange(half), np.arange(grid - half, grid)])
    high = np.arange(half, grid - half)
    assert high.size <= half
    return low, high


def trig(grid):
    n = np.arange(grid)
    angle = ((n[:, None] * n[None, :]) % grid).astype(np.float32) * np.float32(2.0 * math.pi / grid)
    return np.cos(angle), np.sin(angle)


def x_forward(grid, group):
    low, high = lane_order(grid)
    c, s = trig(grid)
    margin = LANES - math.gcd(grid, LANES)
    table = np.zeros((2, margin + 2 * LANES, 3 * LANES), np.float32)
    rows = slice(margin, margin + grid)
    for part in range(2):
        re = c if part == 0 else s
        im = -s if part == 0 else c
        table[part, rows, :LANES] = re[:, low]
        table[part, rows, LANES : 2 * LANES] = im[:, low]
        table[part, rows, 2 * LANES : 2 * LANES + high.size] = re[:, high]
        table[part, rows, 2 * LANES + LANES // 2 : 2 * LANES + LANES // 2 + high.size] = im[:, high]
    return table, margin


def x_backward(grid, group):
    low, high = lane_order(grid)
    c, s = trig(grid)
    table = np.zeros((group, 3 * LANES, 4 * LANES), np.float32)
    for j in range(group):
        off = grid * j % LANES
        re, im = slice(off, off + grid), slice(2 * LANES + off, 2 * LANES + off + grid)
        second = 2 * LANES + LANES // 2
        table[j, :LANES, re], table[j, :LANES, im] = c[low], s[low]
        table[j, LANES : 2 * LANES, re], table[j, LANES : 2 * LANES, im] = -s[low], c[low]
        table[j, 2 * LANES : 2 * LANES + high.size, re] = c[high]
        table[j, 2 * LANES : 2 * LANES + high.size, im] = s[high]
        table[j, second : second + high.size, re] = -s[high]
        table[j, second : second + high.size, im] = c[high]
    return table


def left(grid, sign, outer, inner, padded, order=None):
    c, s = trig(grid)
    table = np.zeros((grid, 2, outer, padded), np.float32)
    table[:, 0, :, :inner] = c.T.reshape(grid, outer, inner)
    table[:, 1, :, :inner] = sign * s.T.reshape(grid, outer, inner)
    table = table.reshape(grid, 2 * outer * padded)
    return table if order is None else table[order]


def turned(re, im, mix):
    lane = lax.broadcasted_iota(jnp.int32, mix.shape, 1)
    rolled = pltpu.roll(mix, LANES // 2, 1)
    swapped = jnp.where(lane < LANES // 2, -rolled, rolled)
    top = jnp.concatenate([re, im, mix], axis=1).astype(BF)
    bottom = jnp.concatenate([-im, re, swapped], axis=1).astype(BF)
    return jnp.concatenate([top, bottom], axis=0)


def dot(a, b):
    return jnp.dot(a, b, preferred_element_type=F32)


def tile(value, t):
    return value[:, t * LANES : (t + 1) * LANES]


def forward_kernel(grid, group, margin, own, rec, wx, fy, out, dens, xs, ys):
    planes = own.shape[2]
    span = grid * group
    count = grid // group
    depth = dens.shape[2]
    tall = up(planes, 8)
    chunk = planes * planes

    def pair(g, _):
        lanes = pl.ds(pl.multiple_of(g * span, LANES), span)
        ur, ui = own[0, 0, :, lanes].astype(F32), own[1, 0, :, lanes].astype(F32)
        rr, ri = rec[0, 0, :, lanes].astype(F32), rec[1, 0, :, lanes].astype(F32)
        dens[0, g, :planes, :] = (rr * ur + ri * ui).astype(BF)
        dens[1, g, :planes, :] = (rr * ui - ri * ur).astype(BF)
        return 0

    lax.fori_loop(0, count, pair, 0)
    step = 8
    for j in range(group):
        start = grid * j // LANES * LANES
        shift = margin - grid * j % LANES
        weight = jnp.concatenate([wx[0, shift : shift + 2 * LANES], wx[1, shift : shift + 2 * LANES]], axis=0)

        def along_x(b, _):
            g0 = b * step
            parts = [dens[p, pl.ds(g0, step), :, start : start + 2 * LANES].reshape(step * depth, 2 * LANES) for p in range(2)]
            got = dot(jnp.concatenate(parts, axis=1), weight)
            for i in range(step):
                for t in range(3):
                    xs[t, pl.ds((g0 + i) * group + j, tall, stride=grid), :] = tile(got[i * depth : i * depth + tall], t)
            return 0

        lax.fori_loop(0, count // step, along_x, 0)

    def along_y(z, _):
        rows = pl.ds(pl.multiple_of(z * grid, 8), grid)
        got = dot(fy[...], turned(xs[0, rows, :], xs[1, rows, :], xs[2, rows, :]))
        for t in range(3):
            ys[t, pl.ds(z, grid, stride=planes), :] = tile(got, t)
        return 0

    lax.fori_loop(0, planes, along_y, 0)
    for d in range(out.shape[0]):
        for t in range(3):
            out[d, t] = ys[t, d * chunk : (d + 1) * chunk, :].astype(BF)


def gathered(held, t, first, planes):
    tall = up(planes, 8)
    return jnp.concatenate([held[s, t, pl.ds(first, tall), :] for s in range(held.shape[0])], axis=0)


def widen(source, held):
    rows = source.shape[2]
    for s in range(source.shape[0]):
        for t in range(3):
            held[s, t, :rows, :] = source[s, t].astype(F32)
            held[s, t, rows:, :] = jnp.zeros((held.shape[2] - rows, LANES), F32)


def column_kernel(grid, planes, source, weights, fz, bz, out, held, cs):
    chunk = planes * planes
    widen(source, held)

    def column(k, _):
        first = k * planes
        got = dot(fz[...], turned(*[gathered(held, t, first, planes) for t in range(3)]))
        low, high = weights[k, :, :LANES], weights[k, :, LANES:]
        scaled = [tile(got, 0) * low, tile(got, 1) * low, tile(got, 2) * high]
        back = dot(bz[...], turned(*scaled))
        for t in range(3):
            cs[t, pl.ds(k, grid, stride=planes), :] = tile(back, t)
        return 0

    lax.fori_loop(0, planes, column, 0)
    for s in range(out.shape[0]):
        for t in range(3):
            out[s, t] = cs[t, s * chunk : (s + 1) * chunk, :].astype(BF)


def backward_kernel(grid, group, source, rec, by, wb, out, held, xs):
    planes = rec.shape[2]
    tall = up(planes, 8)
    span = grid * group
    count = grid // group
    widen(source, held)

    def back_y(z, _):
        got = dot(by[...], turned(*[gathered(held, t, z * planes, planes) for t in range(3)]))
        for t in range(3):
            xs[t, pl.ds(z, grid, stride=tall), :] = tile(got, t)
        return 0

    lax.fori_loop(0, planes, back_y, 0)
    step = 4

    def back_x(b, _):
        tiles = {}
        for j in range(group):
            rows = pl.ds(pl.multiple_of((j * count + b * step) * tall, 8), step * tall)
            got = dot(jnp.concatenate([xs[t, rows, :].astype(BF) for t in range(3)], axis=1), wb[j])
            for part in range(2):
                for side in range(2):
                    key = part, grid * j // LANES + side
                    piece = tile(got, 2 * part + side)
                    tiles[key] = piece if key not in tiles else tiles[key] + piece
        field = [jnp.concatenate([tiles[part, t] for t in range(span // LANES)], axis=1) for part in range(2)]
        for i in range(step):
            lanes = pl.ds(pl.multiple_of((b * step + i) * span, LANES), span)
            fr, fi = [f[i * tall : i * tall + planes] for f in field]
            rr, ri = rec[0, 0, :, lanes].astype(F32), rec[1, 0, :, lanes].astype(F32)
            out[0, 0, :, lanes] = (ri * fi - rr * fr).astype(BF)
            out[1, 0, :, lanes] = (-(rr * fi + ri * fr)).astype(BF)
        return 0

    lax.fori_loop(0, count // step, back_x, 0)


def signed(frequency, grid):
    return jnp.where(frequency >= grid // 2, frequency - grid, frequency)


def weight_table(stick_map, kpoint_grid, grid, planes):
    pool_count, pool_rank = lax.axis_size("pool"), lax.axis_index("pool")
    rows = jnp.arange(pool_count, dtype=jnp.int32)
    earlier = (pool_rank + pool_count - 1) % pool_count
    current = jnp.sum(jnp.where((rows == pool_rank)[:, None], kpoint_grid, 0), axis=0)
    previous = jnp.sum(jnp.where((rows == earlier)[:, None], kpoint_grid, 0), axis=0)
    shift = (current - previous).astype(F32) / KMESH
    low, high = lane_order(grid)
    order = np.full((2 * LANES,), -1, np.int32)
    order[:LANES] = low
    order[LANES : LANES + high.size] = high
    order[LANES + LANES // 2 : LANES + LANES // 2 + high.size] = high
    kx = jnp.asarray(order)
    ky = lax.axis_index("fft") * planes + jnp.arange(planes, dtype=jnp.int32)
    live = stick_map >= 0
    slot_y = jnp.where(live, stick_map // grid, -2)
    slot_x = jnp.where(live, stick_map % grid, -2)
    at_y = (ky[:, None] == slot_y[None, :]).astype(BF)
    at_x = (kx[:, None] == slot_x[None, :]).astype(BF)
    present = lax.dot_general(at_y, at_x, (((1,), (1,)), ((), ())), preferred_element_type=F32) > 0.5
    fx, fy = signed(kx, grid), signed(ky, grid)
    fz = signed(jnp.arange(grid, dtype=jnp.int32), grid)
    radius = grid // 2
    flat = fx[None, :] * fx[None, :] + fy[:, None] * fy[:, None]
    inside = (flat[:, None, :] + (fz * fz)[None, :, None] <= radius * radius) & present[:, None, :]
    wx, wy, wz = [f.astype(F32) + q for f, q in ((fx, shift[0]), (fy, shift[1]), (fz, shift[2]))]
    square = (wz * wz)[None, :, None] + ((wx * wx)[None, :] + (wy * wy)[:, None])[:, None, :]
    square = jnp.where(inside, square, 1.0)
    cell = SPACING_BOHR * grid
    exponent = math.pi * math.pi * square / (cell * cell * SCREENING * SCREENING)
    weights = cell * cell / math.pi * -jnp.expm1(-exponent) / square / float(grid) ** 3
    return jnp.where(inside, weights, 0.0)


def call(kernel, shape, scratch, *args):
    whole = pl.BlockSpec(memory_space=pltpu.VMEM)
    return pl.pallas_call(
        kernel,
        out_shape=jax.ShapeDtypeStruct(shape, BF),
        in_specs=[whole] * len(args),
        out_specs=whole,
        scratch_shapes=scratch,
        compiler_params=pltpu.CompilerParams(vmem_limit_bytes=60 * 2**20),
    )(*args)


def local(orbitals, stick_map, kpoint_grid):
    planes, cells = orbitals.shape[3:]
    grid = math.isqrt(cells)
    group = LANES // math.gcd(grid, LANES)
    count = lax.axis_size("fft")
    pool = lax.axis_size("pool")
    tall = up(planes, 8)
    chunk = planes * planes
    const = lambda table: jnp.asarray(table, dtype=BF)

    rec = lax.ppermute(orbitals, "pool", [(p, (p + 1) % pool) for p in range(pool)])
    weights = weight_table(stick_map, kpoint_grid, grid, planes)
    own, rec = orbitals[0], rec[0]
    wx, margin = x_forward(grid, group)
    fy = left(grid, -1.0, 1, grid, grid)
    sent = call(
        functools.partial(forward_kernel, grid, group, margin),
        (count, 3, chunk, LANES),
        [
            pltpu.VMEM((2, grid // group, up(planes, 16), grid * group), BF),
            pltpu.VMEM((3, tall * grid, LANES), F32),
            pltpu.VMEM((3, planes * grid, LANES), F32),
        ],
        own, rec, const(wx), const(fy),
    )
    landed = lax.all_to_all(sent, "fft", split_axis=0, concat_axis=0, tiled=True)
    held = pltpu.VMEM((count, 3, up(chunk, 8) + 8, LANES), F32)
    returned = call(
        functools.partial(column_kernel, grid, planes),
        (count, 3, chunk, LANES),
        [held, pltpu.VMEM((3, planes * grid, LANES), F32)],
        landed, weights,
        const(left(grid, -1.0, count, planes, tall)),
        const(left(grid, 1.0, 1, grid, grid)),
    )
    back = lax.all_to_all(returned, "fft", split_axis=0, concat_axis=0, tiled=True)
    y_order = np.arange(grid).reshape(grid // group, group).T.reshape(-1)
    result = call(
        functools.partial(backward_kernel, grid, group),
        own.shape,
        [held, pltpu.VMEM((3, tall * grid, LANES), F32)],
        back, rec,
        const(left(grid, 1.0, count, planes, tall, y_order)),
        const(x_backward(grid, group)),
    )
    return result[None]


def solution(mesh):
    return jax.shard_map(
        local,
        mesh=mesh,
        in_specs=(P("pool", None, None, "fft", None), P(), P()),
        out_specs=P("pool", None, None, "fft", None),
        check_vma=False,
    )
```

```python
import functools
import math

import jax
import jax.numpy as jnp
import numpy as np
from jax import lax
from jax.experimental import pallas as pl
from jax.experimental.pallas import tpu as pltpu
from jax.sharding import PartitionSpec as P

KMESH = 4
SPACING_BOHR = 0.1875
SCREENING = 0.106
LANES = 128
BF = jnp.bfloat16
F32 = jnp.float32


def up(value, unit):
    return -(-value // unit) * unit


def lane_order(grid):
    half = LANES // 2
    low = np.concatenate([np.arange(half), np.arange(grid - half, grid)])
    high = np.arange(half, grid - half)
    assert high.size <= half
    return low, high


def trig(grid):
    n = np.arange(grid)
    angle = ((n[:, None] * n[None, :]) % grid).astype(np.float32) * np.float32(2.0 * math.pi / grid)
    return np.cos(angle), np.sin(angle)


def x_forward(grid, group):
    low, high = lane_order(grid)
    c, s = trig(grid)
    margin = LANES - math.gcd(grid, LANES)
    table = np.zeros((2, margin + 2 * LANES, 3 * LANES), np.float32)
    rows = slice(margin, margin + grid)
    for part in range(2):
        re = c if part == 0 else s
        im = -s if part == 0 else c
        table[part, rows, :LANES] = re[:, low]
        table[part, rows, LANES : 2 * LANES] = im[:, low]
        table[part, rows, 2 * LANES : 2 * LANES + high.size] = re[:, high]
        table[part, rows, 2 * LANES + LANES // 2 : 2 * LANES + LANES // 2 + high.size] = im[:, high]
    return table, margin


def x_backward(grid, group):
    low, high = lane_order(grid)
    c, s = trig(grid)
    table = np.zeros((group, 3 * LANES, 4 * LANES), np.float32)
    for j in range(group):
        off = grid * j % LANES
        re, im = slice(off, off + grid), slice(2 * LANES + off, 2 * LANES + off + grid)
        second = 2 * LANES + LANES // 2
        table[j, :LANES, re], table[j, :LANES, im] = c[low], s[low]
        table[j, LANES : 2 * LANES, re], table[j, LANES : 2 * LANES, im] = -s[low], c[low]
        table[j, 2 * LANES : 2 * LANES + high.size, re] = c[high]
        table[j, 2 * LANES : 2 * LANES + high.size, im] = s[high]
        table[j, second : second + high.size, re] = -s[high]
        table[j, second : second + high.size, im] = c[high]
    return table


def left(grid, sign, order=None):
    c, s = trig(grid)
    table = np.concatenate([c.T, sign * s.T], axis=1)
    return table if order is None else table[order]


def cuts(planes):
    return [(first, min(8, planes - first)) for first in range(0, planes, 8)]


def left_cut(grid, sign, outer, planes, order=None):
    c, s = trig(grid)
    blocks = []
    for part in (c.T, sign * s.T):
        part = part.reshape(grid, outer, planes)
        for first, size in cuts(planes):
            block = np.zeros((grid, outer, 8), np.float32)
            block[:, :, :size] = part[:, :, first : first + size]
            blocks.append(block.reshape(grid, outer * 8))
    table = np.concatenate(blocks, axis=1)
    return table if order is None else table[order]


def parcel(planes, size):
    rows = planes * size
    seg = up(rows, 16)
    mixed = rows // 2 if planes % 2 == 0 else rows
    return rows, seg, mixed, 2 * seg + up(mixed, 16)


def turned(re, im, mix):
    lane = lax.broadcasted_iota(jnp.int32, mix.shape, 1)
    rolled = pltpu.roll(mix, LANES // 2, 1)
    swapped = jnp.where(lane < LANES // 2, -rolled, rolled)
    top = jnp.concatenate([re, im, mix], axis=1).astype(BF)
    bottom = jnp.concatenate([-im, re, swapped], axis=1).astype(BF)
    return jnp.concatenate([top, bottom], axis=0)


def dot(a, b):
    return jnp.dot(a, b, preferred_element_type=F32)


def tile(value, t):
    return value[:, t * LANES : (t + 1) * LANES]


def pack(source, first, target, planes, size):
    rows, seg, mixed, total = parcel(planes, size)
    target[:rows, :] = source[0, pl.ds(first, rows), :].astype(BF)
    target[seg : seg + rows, :] = source[1, pl.ds(first, rows), :].astype(BF)
    mix = source[2, pl.ds(first, mixed), :]
    if mixed < rows:
        mix = mix + pltpu.roll(source[2, pl.ds(first + mixed, mixed), :], LANES // 4, 1)
    target[2 * seg : 2 * seg + mixed, :] = mix.astype(BF)


def unpack(source, held, planes, size):
    rows, seg, mixed, total = parcel(planes, size)
    held[0, :rows, :] = source[:rows, :].astype(F32)
    held[1, :rows, :] = source[seg : seg + rows, :].astype(F32)
    mix = source[2 * seg : 2 * seg + mixed, :].astype(F32)
    held[2, :mixed, :] = mix
    if mixed < rows:
        held[2, mixed:rows, :] = pltpu.roll(mix, LANES - LANES // 4, 1)
    spare = held.shape[1] - rows
    for t in range(3):
        held[t, rows:, :] = jnp.zeros((spare, LANES), F32)


def gathered(helds, t, place, planes):
    pieces = []
    for (first, size), held in zip(cuts(planes), helds):
        start = place * size if size % 8 else pl.multiple_of(place * size, 8)
        pieces += [held[s, t, pl.ds(start, 8), :] for s in range(held.shape[0])]
    return jnp.concatenate(pieces, axis=0)


def exchange_kernel(grid, group, margin, pools, *refs):
    own, weights, wx, fy, fz, bz, rec, refs = *refs[:7], refs[7:]
    planes = rec.shape[2]
    parts = cuts(planes)
    n = len(parts)
    backs, refs = refs[:n], refs[n:]
    sends, lands, helds, refs = refs[:n], refs[n : 2 * n], refs[2 * n : 3 * n], refs[3 * n :]
    mine, dens, xs, ys, local_sem, pool_send, pool_recv, out_send, out_recv, in_send, in_recv = refs
    devices = backs[0].shape[0]
    span, count = grid * group, grid // group
    me = lax.axis_index("fft")
    pool = lax.axis_index("pool")
    peers = [lax.rem(me + o, devices) for o in range(1, devices)]
    after, before = lax.rem(pool + 1, pools), lax.rem(pool + pools - 1, pools)

    fetch = pltpu.make_async_copy(own, mine, local_sem)
    fetch.start()
    barrier = pltpu.get_barrier_semaphore()
    targets = [{"fft": peer} for peer in peers] + [{"pool": after}, {"pool": before}]
    for target in targets:
        pl.semaphore_signal(barrier, inc=1, device_id=target, device_id_type=pl.DeviceIdType.MESH)
    pl.semaphore_wait(barrier, len(targets))

    moves = []
    for c, (first, size) in enumerate(parts):
        moves.append(
            pltpu.make_async_remote_copy(
                src_ref=own.at[:, :, pl.ds(first, size), :],
                dst_ref=rec.at[:, :, pl.ds(first, size), :],
                send_sem=pool_send.at[c],
                recv_sem=pool_recv.at[c],
                device_id={"pool": after},
                device_id_type=pl.DeviceIdType.MESH,
            )
        )
        moves[c].start()
    fetch.wait()

    def post(c, source, landing, send_sem, recv_sem):
        copies = []
        for o, peer in enumerate(peers):
            copies.append(
                pltpu.make_async_remote_copy(
                    src_ref=source.at[peer],
                    dst_ref=landing.at[me],
                    send_sem=send_sem.at[c, o],
                    recv_sem=recv_sem.at[c, o],
                    device_id={"fft": peer},
                    device_id_type=pl.DeviceIdType.MESH,
                )
            )
            copies[o].start()
        landing[me] = source[me]
        return copies

    outward, inward = [], []
    for c, (first, size) in enumerate(parts):
        moves[c].wait_recv()
        planes_here = slice(first, first + size)

        def pair(g, _):
            lanes = pl.ds(pl.multiple_of(g * span, LANES), span)
            ur, ui = mine[0, 0, planes_here, lanes].astype(F32), mine[1, 0, planes_here, lanes].astype(F32)
            rr, ri = rec[0, 0, planes_here, lanes].astype(F32), rec[1, 0, planes_here, lanes].astype(F32)
            dens[0, g, :size, :] = rr * ur + ri * ui
            dens[1, g, :size, :] = rr * ui - ri * ur
            return 0

        lax.fori_loop(0, count, pair, 0)
        step = count // 2
        for j in range(group):
            start = grid * j // LANES * LANES
            shift = margin - grid * j % LANES
            weight = jnp.concatenate([wx[0, shift : shift + 2 * LANES], wx[1, shift : shift + 2 * LANES]], axis=0)

            def along_x(b, _):
                g0 = b * step
                sides = [dens[p, pl.ds(g0, step), :, start : start + 2 * LANES].reshape(step * 8, 2 * LANES) for p in range(2)]
                got = dot(jnp.concatenate(sides, axis=1).astype(BF), weight)
                for i in range(step):
                    for t in range(3):
                        xs[t, pl.ds((g0 + i) * group + j, 8, stride=grid), :] = tile(got[i * 8 : i * 8 + 8], t)
                return 0

            lax.fori_loop(0, 2, along_x, 0)

        def along_y(z, _):
            rows = pl.ds(pl.multiple_of(z * grid, 8), grid)
            got = dot(fy[...], turned(xs[0, rows, :], xs[1, rows, :], xs[2, rows, :]))
            for t in range(3):
                ys[t, pl.ds(z, grid, stride=size), :] = tile(got, t)
            return 0

        lax.fori_loop(0, size, along_y, 0)
        for d in range(devices):
            pack(ys, d * planes * size, sends[c].at[d], planes, size)
        outward.append(post(c, sends[c], lands[c], out_send, out_recv))

    for c, (first, size) in enumerate(parts):
        for copy in outward[c]:
            copy.wait_recv()
        for s in range(devices):
            unpack(lands[c].at[s], helds[c].at[s], planes, size)
    for c in range(n):
        for copy in outward[c]:
            copy.wait_send()

    for c, (first, size) in enumerate(parts):

        def column(k, _):
            place = first + k
            got = dot(fz[...], turned(*[gathered(helds, t, place, planes) for t in range(3)]))
            low, high = weights[place, :, :LANES], weights[place, :, LANES:]
            scaled = [tile(got, 0) * low, tile(got, 1) * low, tile(got, 2) * high]
            back = dot(bz[...], turned(*scaled))
            for t in range(3):
                ys[t, pl.ds(k, grid, stride=size), :] = tile(back, t)
            return 0

        lax.fori_loop(0, size, column, 0)
        for d in range(devices):
            pack(ys, d * planes * size, sends[c].at[d], planes, size)
        inward.append(post(c, sends[c], backs[c], in_send, in_recv))

    for c in range(n):
        for copy in inward[c]:
            copy.wait_recv()
            copy.wait_send()
        moves[c].wait_send()


def backward_kernel(grid, group, *refs):
    planes = refs[0].shape[2]
    parts = cuts(planes)
    n = len(parts)
    rec, by, wb, sources, out = refs[0], refs[1], refs[2], refs[3 : 3 + n], refs[3 + n]
    helds, xs = refs[4 + n : 4 + 2 * n], refs[4 + 2 * n]
    tall = up(planes, 8)
    span = grid * group
    count = grid // group

    @pl.when(pl.program_id(0) == 0)
    def _():
        for c, (first, size) in enumerate(parts):
            for s in range(sources[c].shape[0]):
                unpack(sources[c].at[s], helds[c].at[s], planes, size)

        def back_y(z, _):
            got = dot(by[...], turned(*[gathered(helds, t, z, planes) for t in range(3)]))
            for t in range(3):
                xs[t, pl.ds(z, grid, stride=tall), :] = tile(got, t)
            return 0

        lax.fori_loop(0, planes, back_y, 0)

    step = out.shape[3] // span
    tiles = {}
    for j in range(group):
        rows = pl.ds(pl.multiple_of((j * count + pl.program_id(0) * step) * tall, 8), step * tall)
        got = dot(jnp.concatenate([xs[t, rows, :].astype(BF) for t in range(3)], axis=1), wb[j])
        for part in range(2):
            for side in range(2):
                key = part, grid * j // LANES + side
                piece = tile(got, 2 * part + side)
                tiles[key] = piece if key not in tiles else tiles[key] + piece
    field = [jnp.concatenate([tiles[part, t] for t in range(span // LANES)], axis=1) for part in range(2)]
    for i in range(step):
        lanes = slice(i * span, (i + 1) * span)
        fr, fi = [f[i * tall : i * tall + planes] for f in field]
        rr, ri = rec[0, 0, :, lanes].astype(F32), rec[1, 0, :, lanes].astype(F32)
        out[0, 0, :, lanes] = (ri * fi - rr * fr).astype(BF)
        out[1, 0, :, lanes] = (-(rr * fi + ri * fr)).astype(BF)


def signed(frequency, grid):
    return jnp.where(frequency >= grid // 2, frequency - grid, frequency)


def weight_table(stick_map, kpoint_grid, grid, planes):
    pool_count, pool_rank = lax.axis_size("pool"), lax.axis_index("pool")
    rows = jnp.arange(pool_count, dtype=jnp.int32)
    earlier = (pool_rank + pool_count - 1) % pool_count
    current = jnp.sum(jnp.where((rows == pool_rank)[:, None], kpoint_grid, 0), axis=0)
    previous = jnp.sum(jnp.where((rows == earlier)[:, None], kpoint_grid, 0), axis=0)
    shift = (current - previous).astype(F32) / KMESH
    low, high = lane_order(grid)
    order = np.full((2 * LANES,), -1, np.int32)
    order[:LANES] = low
    order[LANES : LANES + high.size] = high
    order[LANES + LANES // 2 : LANES + LANES // 2 + high.size] = high
    kx = jnp.asarray(order)
    ky = lax.axis_index("fft") * planes + jnp.arange(planes, dtype=jnp.int32)
    live = stick_map >= 0
    slot_y = jnp.where(live, stick_map // grid, -2)
    slot_x = jnp.where(live, stick_map % grid, -2)
    at_y = (ky[:, None] == slot_y[None, :]).astype(BF)
    at_x = (kx[:, None] == slot_x[None, :]).astype(BF)
    present = lax.dot_general(at_y, at_x, (((1,), (1,)), ((), ())), preferred_element_type=F32) > 0.5
    fx, fy = signed(kx, grid), signed(ky, grid)
    fz = signed(jnp.arange(grid, dtype=jnp.int32), grid)
    radius = grid // 2
    flat = fx[None, :] * fx[None, :] + fy[:, None] * fy[:, None]
    inside = (flat[:, None, :] + (fz * fz)[None, :, None] <= radius * radius) & present[:, None, :]
    wx, wy, wz = [f.astype(F32) + q for f, q in ((fx, shift[0]), (fy, shift[1]), (fz, shift[2]))]
    square = (wz * wz)[None, :, None] + ((wx * wx)[None, :] + (wy * wy)[:, None])[:, None, :]
    square = jnp.where(inside, square, 1.0)
    cell = SPACING_BOHR * grid
    exponent = math.pi * math.pi * square / (cell * cell * SCREENING * SCREENING)
    weights = cell * cell / math.pi * -jnp.expm1(-exponent) / square / float(grid) ** 3
    return jnp.where(inside, weights, 0.0)


def local(orbitals, stick_map, kpoint_grid):
    planes, cells = orbitals.shape[3:]
    grid = math.isqrt(cells)
    group = LANES // math.gcd(grid, LANES)
    devices = lax.axis_size("fft")
    pools = lax.axis_size("pool")
    const = lambda table: jnp.asarray(table, dtype=BF)
    parts = cuts(planes)
    n = len(parts)
    vmem = pl.BlockSpec(memory_space=pltpu.VMEM)
    parcels = [(devices, parcel(planes, size)[3], LANES) for _, size in parts]
    helds = [pltpu.VMEM((devices, 3, up(planes * size, 8) + 8, LANES), F32) for _, size in parts]
    biggest = max(size for _, size in parts)

    own = orbitals[0]
    weights = weight_table(stick_map, kpoint_grid, grid, planes)
    wx, margin = x_forward(grid, group)
    rec, *backs = pl.pallas_call(
        functools.partial(exchange_kernel, grid, group, margin, pools),
        out_shape=[jax.ShapeDtypeStruct(own.shape, BF)] + [jax.ShapeDtypeStruct(p, BF) for p in parcels],
        in_specs=[pl.BlockSpec(memory_space=pl.ANY)] + [vmem] * 5,
        out_specs=[vmem] * (1 + n),
        scratch_shapes=[pltpu.VMEM(p, BF) for p in parcels]
        + [pltpu.VMEM(p, BF) for p in parcels]
        + helds
        + [
            pltpu.VMEM(own.shape, BF),
            pltpu.VMEM((2, grid // group, 8, grid * group), F32),
            pltpu.VMEM((3, 8 * grid, LANES), F32),
            pltpu.VMEM((3, biggest * grid, LANES), F32),
            pltpu.SemaphoreType.DMA,
            pltpu.SemaphoreType.DMA((n,)),
            pltpu.SemaphoreType.DMA((n,)),
        ]
        + [pltpu.SemaphoreType.DMA((n, devices - 1)) for _ in range(4)],
        compiler_params=pltpu.CompilerParams(vmem_limit_bytes=60 * 2**20, collective_id=0, has_side_effects=True),
    )(own, weights, const(wx), const(left(grid, -1.0)), const(left_cut(grid, -1.0, devices, planes)), const(left(grid, 1.0)))

    y_order = np.arange(grid).reshape(grid // group, group).T.reshape(-1)
    step = 4
    block = pl.BlockSpec(own.shape[:3] + (step * grid * group,), lambda i: (0, 0, 0, i))
    result = pl.pallas_call(
        functools.partial(backward_kernel, grid, group),
        grid=(grid // group // step,),
        out_shape=jax.ShapeDtypeStruct(own.shape, BF),
        in_specs=[block] + [vmem] * (2 + n),
        out_specs=block,
        scratch_shapes=helds + [pltpu.VMEM((3, up(planes, 8) * grid, LANES), F32)],
        compiler_params=pltpu.CompilerParams(vmem_limit_bytes=50 * 2**20),
    )(rec, const(left_cut(grid, 1.0, devices, planes, y_order)), const(x_backward(grid, group)), *backs)
    return result[None]


def solution(mesh):
    return jax.shard_map(
        local,
        mesh=mesh,
        in_specs=(P("pool", None, None, "fft", None), P(), P()),
        out_specs=P("pool", None, None, "fft", None),
        check_vma=False,
    )
```

```python
import functools
import math

import jax
import jax.numpy as jnp
import numpy as np
from jax import lax
from jax.experimental import pallas as pl
from jax.experimental.pallas import tpu as pltpu
from jax.sharding import PartitionSpec as P

KMESH = 4
SPACING_BOHR = 0.1875
SCREENING = 0.106
LANES = 128
BF = jnp.bfloat16
F32 = jnp.float32


def up(value, unit):
    return -(-value // unit) * unit


def lane_order(grid):
    half = LANES // 2
    low = np.concatenate([np.arange(half), np.arange(grid - half, grid)])
    high = np.arange(half, grid - half)
    assert high.size <= half
    return low, high


def trig(grid):
    n = np.arange(grid)
    angle = ((n[:, None] * n[None, :]) % grid).astype(np.float32) * np.float32(2.0 * math.pi / grid)
    return np.cos(angle), np.sin(angle)


def x_forward(grid, group):
    low, high = lane_order(grid)
    c, s = trig(grid)
    margin = LANES - math.gcd(grid, LANES)
    table = np.zeros((2, margin + 2 * LANES, 3 * LANES), np.float32)
    rows = slice(margin, margin + grid)
    for part in range(2):
        re = c if part == 0 else s
        im = -s if part == 0 else c
        table[part, rows, :LANES] = re[:, low]
        table[part, rows, LANES : 2 * LANES] = im[:, low]
        table[part, rows, 2 * LANES : 2 * LANES + high.size] = re[:, high]
        table[part, rows, 2 * LANES + LANES // 2 : 2 * LANES + LANES // 2 + high.size] = im[:, high]
    return table, margin


def x_backward(grid, group):
    low, high = lane_order(grid)
    c, s = trig(grid)
    table = np.zeros((group, 3 * LANES, 4 * LANES), np.float32)
    for j in range(group):
        off = grid * j % LANES
        re, im = slice(off, off + grid), slice(2 * LANES + off, 2 * LANES + off + grid)
        second = 2 * LANES + LANES // 2
        table[j, :LANES, re], table[j, :LANES, im] = c[low], s[low]
        table[j, LANES : 2 * LANES, re], table[j, LANES : 2 * LANES, im] = -s[low], c[low]
        table[j, 2 * LANES : 2 * LANES + high.size, re] = c[high]
        table[j, 2 * LANES : 2 * LANES + high.size, im] = s[high]
        table[j, second : second + high.size, re] = -s[high]
        table[j, second : second + high.size, im] = c[high]
    return table


def left(grid, sign, order=None):
    c, s = trig(grid)
    table = np.concatenate([c.T, sign * s.T], axis=1)
    return table if order is None else table[order]


def cuts(planes):
    return [(first, min(8, planes - first)) for first in range(0, planes, 8)]


def left_cut(grid, sign, outer, planes, order=None):
    c, s = trig(grid)
    blocks = []
    for part in (c.T, sign * s.T):
        part = part.reshape(grid, outer, planes)
        for first, size in cuts(planes):
            block = np.zeros((grid, outer, 8), np.float32)
            block[:, :, :size] = part[:, :, first : first + size]
            blocks.append(block.reshape(grid, outer * 8))
    table = np.concatenate(blocks, axis=1)
    return table if order is None else table[order]


def parcel(planes, size):
    rows = planes * size
    seg = up(rows, 16)
    mixed = rows // 2 if planes % 2 == 0 else rows
    return rows, seg, mixed, 2 * seg + up(mixed, 16)


def turned(re, im, mix):
    lane = lax.broadcasted_iota(jnp.int32, mix.shape, 1)
    rolled = pltpu.roll(mix, LANES // 2, 1)
    swapped = jnp.where(lane < LANES // 2, -rolled, rolled)
    top = jnp.concatenate([re, im, mix], axis=1).astype(BF)
    bottom = jnp.concatenate([-im, re, swapped], axis=1).astype(BF)
    return jnp.concatenate([top, bottom], axis=0)


def dot(a, b):
    return jnp.dot(a, b, preferred_element_type=F32)


def tile(value, t):
    return value[:, t * LANES : (t + 1) * LANES]


def pack(source, first, target, planes, size):
    rows, seg, mixed, total = parcel(planes, size)
    target[:rows, :] = source[0, pl.ds(first, rows), :].astype(BF)
    target[seg : seg + rows, :] = source[1, pl.ds(first, rows), :].astype(BF)
    mix = source[2, pl.ds(first, mixed), :]
    if mixed < rows:
        mix = mix + pltpu.roll(source[2, pl.ds(first + mixed, mixed), :], LANES // 4, 1)
    target[2 * seg : 2 * seg + mixed, :] = mix.astype(BF)


def unpack(source, held, planes, size):
    rows, seg, mixed, total = parcel(planes, size)
    held[0, :rows, :] = source[:rows, :].astype(F32)
    held[1, :rows, :] = source[seg : seg + rows, :].astype(F32)
    mix = source[2 * seg : 2 * seg + mixed, :].astype(F32)
    held[2, :mixed, :] = mix
    if mixed < rows:
        held[2, mixed:rows, :] = pltpu.roll(mix, LANES - LANES // 4, 1)
    spare = held.shape[1] - rows
    for t in range(3):
        held[t, rows:, :] = jnp.zeros((spare, LANES), F32)


def gathered(helds, t, place, planes):
    pieces = []
    for (first, size), held in zip(cuts(planes), helds):
        start = place * size if size % 8 else pl.multiple_of(place * size, 8)
        pieces += [held[s, t, pl.ds(start, 8), :] for s in range(held.shape[0])]
    return jnp.concatenate(pieces, axis=0)


def exchange_kernel(grid, group, margin, pools, *refs):
    own, slots, kx_rows, kx_lanes, q, wx, fy, fz, bz, rec, refs = *refs[:10], refs[10:]
    weights, present, refs = refs[-2], refs[-1], refs[:-2]
    planes = rec.shape[2]
    parts = cuts(planes)
    n = len(parts)
    backs, refs = refs[:n], refs[n:]
    sends, lands, helds, refs = refs[:n], refs[n : 2 * n], refs[2 * n : 3 * n], refs[3 * n :]
    mine, dens, xs, ys, local_sem, pool_send, pool_recv, out_send, out_recv, in_send, in_recv = refs
    devices = backs[0].shape[0]
    span, count = grid * group, grid // group
    me = lax.axis_index("fft")
    pool = lax.axis_index("pool")
    peers = [lax.rem(me + o, devices) for o in range(1, devices)]
    after, before = lax.rem(pool + 1, pools), lax.rem(pool + pools - 1, pools)

    fetch = pltpu.make_async_copy(own, mine, local_sem)
    fetch.start()
    barrier = pltpu.get_barrier_semaphore()
    targets = [{"fft": peer} for peer in peers] + [{"pool": after}, {"pool": before}]
    for target in targets:
        pl.semaphore_signal(barrier, inc=1, device_id=target, device_id_type=pl.DeviceIdType.MESH)
    pl.semaphore_wait(barrier, len(targets))

    moves = []
    for c, (first, size) in enumerate(parts):
        moves.append(
            pltpu.make_async_remote_copy(
                src_ref=own.at[:, :, pl.ds(first, size), :],
                dst_ref=rec.at[:, :, pl.ds(first, size), :],
                send_sem=pool_send.at[c],
                recv_sem=pool_recv.at[c],
                device_id={"pool": after},
                device_id_type=pl.DeviceIdType.MESH,
            )
        )
        moves[c].start()
    fetch.wait()
    fill_weights(grid, planes, me * planes, slots, kx_rows, kx_lanes, q, present, weights)

    def post(c, source, landing, send_sem, recv_sem):
        copies = []
        for o, peer in enumerate(peers):
            copies.append(
                pltpu.make_async_remote_copy(
                    src_ref=source.at[peer],
                    dst_ref=landing.at[me],
                    send_sem=send_sem.at[c, o],
                    recv_sem=recv_sem.at[c, o],
                    device_id={"fft": peer},
                    device_id_type=pl.DeviceIdType.MESH,
                )
            )
            copies[o].start()
        landing[me] = source[me]
        return copies

    outward, inward = [], []
    for c, (first, size) in enumerate(parts):
        moves[c].wait_recv()
        planes_here = slice(first, first + size)

        def pair(g, _):
            lanes = pl.ds(pl.multiple_of(g * span, LANES), span)
            ur, ui = mine[0, 0, planes_here, lanes].astype(F32), mine[1, 0, planes_here, lanes].astype(F32)
            rr, ri = rec[0, 0, planes_here, lanes].astype(F32), rec[1, 0, planes_here, lanes].astype(F32)
            dens[0, g, :size, :] = rr * ur + ri * ui
            dens[1, g, :size, :] = rr * ui - ri * ur
            return 0

        lax.fori_loop(0, count, pair, 0)
        step = count // 2
        for j in range(group):
            start = grid * j // LANES * LANES
            shift = margin - grid * j % LANES
            weight = jnp.concatenate([wx[0, shift : shift + 2 * LANES], wx[1, shift : shift + 2 * LANES]], axis=0)

            def along_x(b, _):
                g0 = b * step
                sides = [dens[p, pl.ds(g0, step), :, start : start + 2 * LANES].reshape(step * 8, 2 * LANES) for p in range(2)]
                got = dot(jnp.concatenate(sides, axis=1).astype(BF), weight)
                for i in range(step):
                    for t in range(3):
                        xs[t, pl.ds((g0 + i) * group + j, 8, stride=grid), :] = tile(got[i * 8 : i * 8 + 8], t)
                return 0

            lax.fori_loop(0, 2, along_x, 0)

        def along_y(z, _):
            rows = pl.ds(pl.multiple_of(z * grid, 8), grid)
            got = dot(fy[...], turned(xs[0, rows, :], xs[1, rows, :], xs[2, rows, :]))
            for t in range(3):
                ys[t, pl.ds(z, grid, stride=size), :] = tile(got, t)
            return 0

        lax.fori_loop(0, size, along_y, 0)
        for d in range(devices):
            pack(ys, d * planes * size, sends[c].at[d], planes, size)
        outward.append(post(c, sends[c], lands[c], out_send, out_recv))

    for c, (first, size) in enumerate(parts):
        for copy in outward[c]:
            copy.wait_recv()
        for s in range(devices):
            unpack(lands[c].at[s], helds[c].at[s], planes, size)
    for c in range(n):
        for copy in outward[c]:
            copy.wait_send()

    for c, (first, size) in enumerate(parts):

        def column(k, _):
            place = first + k
            got = dot(fz[...], turned(*[gathered(helds, t, place, planes) for t in range(3)]))
            low, high = weights[place, :, :LANES], weights[place, :, LANES:]
            scaled = [tile(got, 0) * low, tile(got, 1) * low, tile(got, 2) * high]
            back = dot(bz[...], turned(*scaled))
            for t in range(3):
                ys[t, pl.ds(k, grid, stride=size), :] = tile(back, t)
            return 0

        lax.fori_loop(0, size, column, 0)
        for d in range(devices):
            pack(ys, d * planes * size, sends[c].at[d], planes, size)
        inward.append(post(c, sends[c], backs[c], in_send, in_recv))

    for c in range(n):
        for copy in inward[c]:
            copy.wait_recv()
            copy.wait_send()
        moves[c].wait_send()


def backward_kernel(grid, group, *refs):
    planes = refs[0].shape[2]
    parts = cuts(planes)
    n = len(parts)
    rec, by, wb, sources, out = refs[0], refs[1], refs[2], refs[3 : 3 + n], refs[3 + n]
    helds, xs = refs[4 + n : 4 + 2 * n], refs[4 + 2 * n]
    tall = up(planes, 8)
    span = grid * group
    count = grid // group

    @pl.when(pl.program_id(0) == 0)
    def _():
        for c, (first, size) in enumerate(parts):
            for s in range(sources[c].shape[0]):
                unpack(sources[c].at[s], helds[c].at[s], planes, size)

        def back_y(z, _):
            got = dot(by[...], turned(*[gathered(helds, t, z, planes) for t in range(3)]))
            for t in range(3):
                xs[t, pl.ds(z, grid, stride=tall), :] = tile(got, t)
            return 0

        lax.fori_loop(0, planes, back_y, 0)

    step = out.shape[3] // span
    tiles = {}
    for j in range(group):
        rows = pl.ds(pl.multiple_of((j * count + pl.program_id(0) * step) * tall, 8), step * tall)
        got = dot(jnp.concatenate([xs[t, rows, :].astype(BF) for t in range(3)], axis=1), wb[j])
        for part in range(2):
            for side in range(2):
                key = part, grid * j // LANES + side
                piece = tile(got, 2 * part + side)
                tiles[key] = piece if key not in tiles else tiles[key] + piece
    field = [jnp.concatenate([tiles[part, t] for t in range(span // LANES)], axis=1) for part in range(2)]
    for i in range(step):
        lanes = slice(i * span, (i + 1) * span)
        fr, fi = [f[i * tall : i * tall + planes] for f in field]
        rr, ri = rec[0, 0, :, lanes].astype(F32), rec[1, 0, :, lanes].astype(F32)
        out[0, 0, :, lanes] = (ri * fi - rr * fr).astype(BF)
        out[1, 0, :, lanes] = (-(rr * fi + ri * fr)).astype(BF)


def signed(frequency, grid):
    return jnp.where(frequency >= grid // 2, frequency - grid, frequency)


def spectral_kx(grid):
    low, high = lane_order(grid)
    order = np.full((2 * LANES,), -1, np.int32)
    order[:LANES] = low
    order[LANES : LANES + high.size] = high
    order[LANES + LANES // 2 : LANES + LANES // 2 + high.size] = high
    return order


def fill_weights(grid, planes, first_ky, slots, kx_rows, kx_lanes, shift, present, weights):
    tall = present.shape[0]
    width = slots.shape[1] // 5
    present[...] = jnp.zeros(present.shape, F32)
    ky = first_ky + lax.broadcasted_iota(jnp.int32, (tall, width), 0)

    def find(i, _):
        lanes = pl.ds(pl.multiple_of(i * width, LANES), width)
        at_y = jnp.where(ky == slots[0:1, lanes], 1.0, 0.0).astype(BF)
        at_x = jnp.where(kx_rows[...] == slots[1:2, lanes], 1.0, 0.0).astype(BF)
        present[...] += lax.dot_general(at_y, at_x, (((1,), (1,)), ((), ())), preferred_element_type=F32)
        return 0

    lax.fori_loop(0, 5, find, 0)
    shape = (grid, 2 * LANES)
    fx = signed(jnp.broadcast_to(kx_lanes[...], shape), grid)
    fz = signed(lax.broadcasted_iota(jnp.int32, shape, 0), grid)
    wx = fx.astype(F32) + shift[0:1, :]
    wz = fz.astype(F32) + shift[2:3, :]
    flat = fx * fx + fz * fz
    partial = wz * wz + wx * wx
    radius = grid // 2
    cell = SPACING_BOHR * grid
    rate = math.pi * math.pi / (cell * cell * SCREENING * SCREENING)
    scale = cell * cell / math.pi / float(grid) ** 3

    def fill(k, _):
        fy = signed(first_ky + k, grid)
        wy = fy.astype(F32) + shift[1:2, :]
        inside = (flat + fy * fy <= radius * radius) & (present[pl.ds(k, 1), :] > 0.5)
        square = jnp.where(inside, partial + wy * wy, 1.0)
        weights[k] = jnp.where(inside, scale * (1.0 - jnp.exp(-rate * square)) / square, 0.0)
        return 0

    lax.fori_loop(0, planes, fill, 0)


def local(orbitals, stick_map, kpoint_grid):
    planes, cells = orbitals.shape[3:]
    grid = math.isqrt(cells)
    group = LANES // math.gcd(grid, LANES)
    devices = lax.axis_size("fft")
    pools = lax.axis_size("pool")
    const = lambda table: jnp.asarray(table, dtype=BF)
    parts = cuts(planes)
    n = len(parts)
    vmem = pl.BlockSpec(memory_space=pltpu.VMEM)
    parcels = [(devices, parcel(planes, size)[3], LANES) for _, size in parts]
    helds = [pltpu.VMEM((devices, 3, up(planes * size, 8) + 8, LANES), F32) for _, size in parts]
    biggest = max(size for _, size in parts)

    own = orbitals[0]
    pool_rank = lax.axis_index("pool")
    ranks = jnp.arange(pools, dtype=jnp.int32)
    earlier = (pool_rank + pools - 1) % pools
    sign = (ranks == pool_rank).astype(jnp.int32) - (ranks == earlier).astype(jnp.int32)
    q = jnp.sum(sign[:, None] * kpoint_grid, axis=0).astype(F32) / KMESH
    q = jnp.broadcast_to(q[:, None], (3, 2 * LANES))
    live = stick_map >= 0
    slots = jnp.stack([jnp.where(live, stick_map // grid, -2), jnp.where(live, stick_map % grid, -2)])
    slots = jnp.pad(slots, ((0, 0), (0, -slots.shape[1] % (5 * LANES))), constant_values=-2)
    kx = spectral_kx(grid)
    wx, margin = x_forward(grid, group)
    rec, *backs = pl.pallas_call(
        functools.partial(exchange_kernel, grid, group, margin, pools),
        out_shape=[jax.ShapeDtypeStruct(own.shape, BF)] + [jax.ShapeDtypeStruct(p, BF) for p in parcels],
        in_specs=[pl.BlockSpec(memory_space=pl.ANY)] + [vmem] * 8,
        out_specs=[vmem] * (1 + n),
        scratch_shapes=[pltpu.VMEM(p, BF) for p in parcels]
        + [pltpu.VMEM(p, BF) for p in parcels]
        + helds
        + [
            pltpu.VMEM(own.shape, BF),
            pltpu.VMEM((2, grid // group, 8, grid * group), F32),
            pltpu.VMEM((3, 8 * grid, LANES), F32),
            pltpu.VMEM((3, biggest * grid, LANES), F32),
            pltpu.SemaphoreType.DMA,
            pltpu.SemaphoreType.DMA((n,)),
            pltpu.SemaphoreType.DMA((n,)),
        ]
        + [pltpu.SemaphoreType.DMA((n, devices - 1)) for _ in range(4)]
        + [pltpu.VMEM((planes, grid, 2 * LANES), F32), pltpu.VMEM((up(planes, 8), 2 * LANES), F32)],
        compiler_params=pltpu.CompilerParams(vmem_limit_bytes=60 * 2**20, collective_id=0, has_side_effects=True),
    )(own, slots, jnp.asarray(kx[:, None]), jnp.asarray(kx[None, :]), q, const(wx), const(left(grid, -1.0)), const(left_cut(grid, -1.0, devices, planes)), const(left(grid, 1.0)))

    y_order = np.arange(grid).reshape(grid // group, group).T.reshape(-1)
    step = 4
    block = pl.BlockSpec(own.shape[:3] + (step * grid * group,), lambda i: (0, 0, 0, i))
    result = pl.pallas_call(
        functools.partial(backward_kernel, grid, group),
        grid=(grid // group // step,),
        out_shape=jax.ShapeDtypeStruct(own.shape, BF),
        in_specs=[block] + [vmem] * (2 + n),
        out_specs=block,
        scratch_shapes=helds + [pltpu.VMEM((3, up(planes, 8) * grid, LANES), F32)],
        compiler_params=pltpu.CompilerParams(vmem_limit_bytes=50 * 2**20),
    )(rec, const(left_cut(grid, 1.0, devices, planes, y_order)), const(x_backward(grid, group)), *backs)
    return result[None]


def solution(mesh):
    return jax.shard_map(
        local,
        mesh=mesh,
        in_specs=(P("pool", None, None, "fft", None), P(), P()),
        out_specs=P("pool", None, None, "fft", None),
        check_vma=False,
    )
```
